256 devices in a mesh: dp: 8 (over x, core), expert: 32 (over z, y).
Axes of the slice: x: 4, y: 4, z: 8, core: 2. Of those that a mesh axis runs over, the one named last changes fastest.
Arguments:
- tokens: bfloat16 [5120, 262144], P(None, ('dp', 'expert')), may hold values from -24 to 24, as said below
- router: bfloat16 [5120, 160], P(None, 'expert'), may hold values from -1 to 1, as said below
- device_pick: int32 [3, 262144], P(None, 'dp'), may hold values from 0 to 31, as said below
- expert_pick: int32 [6, 262144], P(None, 'dp'), may hold values from 0 to 159, as said below
Outputs:
- gates: float32 [6, 262144], P(None, 'dp')
- device_max: float32 [32, 262144], P('expert', 'dp')
- balance: float32 [3], replicated
The draws below stay inside these ranges and needn't reach their ends.
Inputs may be any that keep to these rules, and one draw needn't show every extreme that they name: tokens lie within the range; in each column the values are of order one, except in a few columns. router entries are of order 1 / sqrt(5120). `device_pick`: each column names 3 different devices. `expert_pick`: each column names 6 different experts, two on each device of the column's device_pick, in that order; the device of expert e is e // 5.
All inputs are finite; a program needn't handle non-finite values.
Results may differ from the reference program's by a relative error of at most 0.0003.
Values may be sent and summed in bfloat16 or wider, within the bound.
A program may use at most 64 MiB of HBM per device.

```python
import jax
import jax.numpy as jnp
from jax import lax

D = 5120
EXP_DEV = 5
TOP = 6
DEV_TOP = 3
TOK_DEV = 32768
NDEV = 32
E = 160
TOKENS = 262144


def router_base(key):
    values = jax.random.normal(jax.random.fold_in(key, 7), (D, E), jnp.float32)
    return jnp.clip(values, -6.0, 6.0) * D ** (-0.5)


def draw_router(key, part):
    return router_base(key).astype(jnp.bfloat16)


def draw_tokens(key, part):
    inner = jax.random.fold_in(key, 3)
    shared = jax.random.normal(jax.random.fold_in(inner, 1), (D,), jnp.float32) * 0.5
    values = jax.random.normal(jax.random.fold_in(inner, 4), (TOKENS, D), jnp.float32) + shared[None, :]
    return jnp.clip(values, -24.0, 24.0).T.astype(jnp.bfloat16)


def draw_picks(key):
    inner = jax.random.fold_in(key, 11)
    span = max(TOK_DEV // 2, 1)
    blocks = (TOKENS + span - 1) // span
    hot_table = jax.random.randint(jax.random.fold_in(inner, 1), (blocks, 4), 0, NDEV)
    rows = jnp.arange(TOKENS, dtype=jnp.int32)
    hot_rows = hot_table[rows // span]
    slots = jnp.arange(NDEV, dtype=jnp.int32)
    hot = jnp.any(hot_rows[:, :, None] == slots[None, None, :], axis=1).astype(jnp.int32)
    noise = jax.random.randint(jax.random.fold_in(inner, 2), (TOKENS, NDEV), 0, 2 ** 22)
    keyed = (noise + hot * 2 ** 21) * NDEV + slots[None, :]
    _, chosen_dev = lax.top_k(keyed, DEV_TOP)
    chosen_dev = chosen_dev.astype(jnp.int32)
    local_noise = jax.random.randint(jax.random.fold_in(inner, 3), (TOKENS, DEV_TOP, EXP_DEV), 0, 2 ** 20)
    local_keyed = local_noise * EXP_DEV + jnp.arange(EXP_DEV, dtype=jnp.int32)[None, None, :]
    _, local_slot = lax.top_k(local_keyed, 2)
    experts = chosen_dev[:, :, None] * EXP_DEV + local_slot.astype(jnp.int32)
    return (chosen_dev.T, experts.reshape(TOKENS, TOP).T.astype(jnp.int32))


def draw_device_pick(key, part):
    return draw_picks(key)[0]


def draw_expert_pick(key, part):
    return draw_picks(key)[1]


def setup_inputs(seed: int = 0) -> dict:
    keys = jax.random.split(jax.random.key(seed), 5)
    tokens = draw_tokens(jax.random.fold_in(keys[4], 71), 0)
    router = draw_router(jax.random.fold_in(keys[4], 71), 0)
    device_pick = draw_device_pick(jax.random.fold_in(keys[4], 71), 0)
    expert_pick = draw_expert_pick(jax.random.fold_in(keys[4], 71), 0)
    return {"tokens": tokens, "router": router, "device_pick": device_pick, "expert_pick": expert_pick}


def reference(tokens, router, device_pick, expert_pick):
    scores = jnp.dot(router.T, tokens, preferred_element_type=jnp.float32)
    peak = jnp.max(scores, axis=0, keepdims=True)
    raised = jnp.exp(scores - peak)
    probs = raised / jnp.sum(raised, axis=0, keepdims=True)
    gates = jnp.take_along_axis(probs, expert_pick, axis=0)
    device_max = jnp.max(probs.reshape(NDEV, EXP_DEV, TOKENS), axis=1)
    ones_exp = jnp.ones((TOKENS * TOP,), jnp.float32)
    counts = jax.ops.segment_sum(ones_exp, expert_pick.reshape(-1), num_segments=E)
    ones_dev = jnp.ones((TOKENS * DEV_TOP,), jnp.float32)
    sent_counts = jax.ops.segment_sum(ones_dev, device_pick.reshape(-1), num_segments=NDEV)
    freq = counts * (E / (TOP * TOKENS))
    prob = jnp.sum(probs, axis=1) / TOKENS
    dev_freq = jnp.mean(freq.reshape(NDEV, EXP_DEV), axis=1)
    dev_prob = jnp.sum(prob.reshape(NDEV, EXP_DEV), axis=1)
    sent = sent_counts * (NDEV / (DEV_TOP * TOKENS))
    balance = jnp.stack([jnp.sum(freq * prob), jnp.sum(dev_freq * dev_prob), jnp.sum(sent * dev_prob)])
    return gates, device_max, balance
```

```python
import jax
import jax.numpy as jnp
from jax import lax
from jax.experimental import pallas as pl
from jax.experimental.pallas import tpu as pltpu
from jax.sharding import PartitionSpec as P

MESH = pl.DeviceIdType.MESH
TOP = 6
DEV_TOP = 3
PER = 5
NX, NZ, NY = 4, 8, 4
NDP = 2 * NX
NDEV = NZ * NY
CODE = 1.4426950408889634 * 2048.0
NEG = -1e30
WORDS = TOP // 2
CHUNKS = 2
Z_ORDER = (1, 7, 2, 6, 3, 5, 4)
Y_ORDER = (1, 3, 2)


def rem(a, b):
    return lax.rem(a, b)


def encode(log_norm, value):
    return jnp.clip((log_norm - value) * CODE + 0.5, 0.0, 65535.0).astype(jnp.int32)


def low_half(words):
    return jnp.exp2((words & 65535).astype(jnp.float32) * (-1.0 / 2048.0))


def high_half(words):
    return jnp.exp2(lax.shift_right_logical(words, 16).astype(jnp.float32) * (-1.0 / 2048.0))


def kernel(
    tokens, router, device_pick, expert_pick,
    gates, device_max, balance,
    tok, raw, picks, dpicks, main, tail, lhs, part, prob_acc, top_code, gate_msg, top_msg, top_recv,
    cnt_dp, cnt_all, bal_dp, bal_z, bal_y,
    in_sem, tok_sem, zs, zr, ys, yr, cs, cr, ks, kr, gzs, gzr, gys, gyr, ts, tr, bs, br,
):
    depth, share = tokens.shape
    half, width = depth // 2, share // CHUNKS
    quarter = depth // 4
    total = share * NDEV * NDP
    dp, me = lax.axis_index("dp"), lax.axis_index("expert")
    core, z, y = rem(dp, 2), me // NY, rem(me, NY)
    partner = dp + 1 - 2 * core

    def zz(j):
        return rem(z + NZ - j, NZ)

    def yy(q):
        return rem(y + NY - q, NY)

    def z_peer(j):
        return (dp, rem(z + j, NZ) * NY + y)

    def y_peer(q):
        return (dp, z * NY + rem(y + q, NY))

    def dp_peer(i):
        return (rem(dp + i, NDP), me)

    def send(src, dst, s, r, device):
        return pltpu.make_async_remote_copy(
            src_ref=src, dst_ref=dst, send_sem=s, recv_sem=r, device_id=device, device_id_type=MESH
        )

    raw_copy = pltpu.make_async_copy(router, raw, in_sem.at[0])
    pick_copy = pltpu.make_async_copy(expert_pick, picks, in_sem.at[1])
    dpick_copy = pltpu.make_async_copy(device_pick, dpicks, in_sem.at[2])
    raw_copy.start()
    pick_copy.start()
    dpick_copy.start()

    def token_copy(c):
        return pltpu.make_async_copy(tokens.at[:, pl.ds(c * width, width)], tok.at[c], tok_sem.at[c])

    for c in range(CHUNKS):
        token_copy(c).start()

    barrier = pltpu.get_barrier_semaphore()
    friends = [z_peer(j) for j in Z_ORDER] + [y_peer(q) for q in Y_ORDER] + [dp_peer(i) for i in range(1, NDP)]
    for device in friends:
        pl.semaphore_signal(barrier, inc=1, device_id=device, device_id_type=MESH)

    def tail_slot(zi, yi):
        return zi * NY + rem(yi, 2) * 2 + yi // 2

    raw_copy.wait()
    main[me] = raw[0:4, :]
    last = raw[4:5, :].astype(jnp.float32)
    tail[tail_slot(z, y)] = jnp.concatenate(
        [
            jnp.concatenate([last[:, 0:quarter], last[:, 2 * quarter : 3 * quarter]], axis=1),
            jnp.concatenate([last[:, quarter : 2 * quarter], last[:, 3 * quarter :]], axis=1),
        ],
        axis=0,
    ).astype(jnp.bfloat16)

    pick_copy.wait()
    dpick_copy.wait()
    one, nil = jnp.float32(1.0), jnp.float32(0.0)

    def count(i, carry):
        counts, sends = carry
        counts = list(counts)
        for b in range(8):
            cols = pl.ds(pl.multiple_of(i * 1024 + b * 128, 128), 128)
            seen = picks[:, cols] - me * PER
            for e in range(PER):
                counts[e] = counts[e] + jnp.where(seen == e, one, nil)
            sends = sends + jnp.where(dpicks[:, cols] == me, one, nil)
        return tuple(counts), sends

    counts, sends = lax.fori_loop(
        0,
        share * NDEV // 1024,
        count,
        (tuple(jnp.zeros((TOP, 128), jnp.float32) for _ in range(PER)), jnp.zeros((DEV_TOP, 128), jnp.float32)),
    )
    lane = lax.broadcasted_iota(jnp.int32, (1, 128), 1)

    def whole(v):
        return jnp.sum(jnp.sum(v, axis=0, keepdims=True), axis=1, keepdims=True)

    mine = jnp.where(lane == PER, whole(sends), nil)
    for e in range(PER):
        mine = jnp.where(lane == e, whole(counts[e]), mine)
    cnt_dp[dp] = mine

    pl.semaphore_wait(barrier, len(friends))

    def main_at(zi, yi, c):
        return main.at[zi * NY + yi, :, pl.ds(pl.multiple_of(c * half, half), half)]

    def tail_at(zi, yi, c):
        return tail.at[tail_slot(zi, yi), :, pl.ds(pl.multiple_of(c * quarter, quarter), quarter)]

    def z_copies(j, mine=True):
        zi = z if mine else zz(j)
        return [
            send(f(zi, y, core), f(zi, y, core), zs.at[n, j], zr.at[n, j], z_peer(j))
            for n, f in enumerate((main_at, tail_at))
        ]

    def y_copies(q, j, mine=True):
        yi = y if mine else yy(q)
        return [
            send(f(zz(j), yi, core), f(zz(j), yi, core), ys.at[n, q, j], yr.at[n, q, j], y_peer(q))
            for n, f in enumerate((main_at, tail_at))
        ]

    def core_copies(q, j, c):
        return [
            send(f(zz(j), yy(q), c), f(zz(j), yy(q), c), cs.at[n, q, j], cr.at[n, q, j], (partner, me))
            for n, f in enumerate((main_at, tail_at))
        ]

    def start(copies):
        for copy in copies:
            copy.start()

    def arrive(copies):
        for copy in copies:
            copy.wait_recv()

    for j in Z_ORDER:
        start(z_copies(j))
    for q in Y_ORDER:
        start(y_copies(q, 0))
    cnt_copies = [send(cnt_dp.at[dp], cnt_dp.at[dp], ks.at[0, i], kr.at[0, i], dp_peer(i)) for i in range(1, NDP)]
    start(cnt_copies)
    for j in Z_ORDER:
        arrive(z_copies(j, False))
        for q in Y_ORDER:
            start(y_copies(q, j))
        start(core_copies(0, j, core))

    arrive(cnt_copies)
    cnt_all[y, z] = jnp.sum(cnt_dp[...], axis=0)
    for q in Y_ORDER:
        arrive(y_copies(q, 0, False))
        start(core_copies(q, 0, core))
    cnt_z = [send(cnt_all.at[y, z], cnt_all.at[y, z], ks.at[1, j], kr.at[1, j], z_peer(j)) for j in range(1, NZ)]
    start(cnt_z)
    for n, j in enumerate(Z_ORDER):
        for q in Y_ORDER:
            arrive(y_copies(q, j, False))
            start(core_copies(q, j, core))
        if n == 4:
            arrive([send(cnt_all.at[y, zz(j)], cnt_all.at[y, zz(j)], ks.at[1, j], kr.at[1, j], z_peer(j)) for j in range(1, NZ)])
            cnt_y = [send(cnt_all.at[y], cnt_all.at[y], ks.at[2, q], kr.at[2, q], y_peer(q)) for q in Y_ORDER]
            start(cnt_y)
    for j in (0,) + Z_ORDER:
        for q in (0,) + Y_ORDER:
            if j or q:
                arrive(core_copies(q, j, 1 - core))

    block = 512
    for i in range(depth // block):
        lhs[0 : 4 * NDEV, i * block : (i + 1) * block] = main[:, :, i * block : (i + 1) * block].reshape(4 * NDEV, block)
    for h in range(2):
        for i in range(quarter // 256):
            piece = tail[:, :, h * quarter + i * 256 : h * quarter + (i + 1) * 256].reshape(2 * NDEV, 256)
            for s in range(2):
                at = (2 * h + s) * quarter + i * 256
                lhs[4 * NDEV :, at : at + 256] = piece

    row = lax.broadcasted_iota(jnp.int32, (4 * NDEV, 128), 0)
    ids = (row // 4) * PER + rem(row, 4)
    trow = lax.broadcasted_iota(jnp.int32, (2 * NDEV, 128), 0)
    tdev = (trow // 8) * NY + rem(trow // 2, 2) * 2 + rem(trow // 4, 2)
    even = rem(trow, 2) == 0
    tail_ids = jnp.where(even, tdev * PER + PER - 1, -1)
    row8 = lax.broadcasted_iota(jnp.int32, (NZ, 8, 128), 1)
    prob_acc[...] = jnp.zeros((6 * NDEV, 128), jnp.float32)

    def gate_at(src, c):
        return gate_msg.at[src, c]

    def gate_z(j, c, mine=True):
        src = me if mine else zz(j) * NY + y
        return send(gate_at(src, c), gate_at(src, c), gzs.at[j, c], gzr.at[j, c], z_peer(j))

    def gate_y(q, j, c, mine=True):
        src = zz(j) * NY + (y if mine else yy(q))
        return send(gate_at(src, c), gate_at(src, c), gys.at[q, j, c], gyr.at[q, j, c], y_peer(q))

    for c in range(CHUNKS):
        token_copy(c).wait()
        dots = [
            jnp.dot(
                lhs[:, s * quarter : (s + 1) * quarter],
                tok[c, s * quarter : (s + 1) * quarter, :],
                preferred_element_type=jnp.float32,
            )
            for s in range(4)
        ]
        split = 4 * NDEV
        part[0:split, :] = (dots[0][:split] + dots[1][:split]) + (dots[2][:split] + dots[3][:split])
        part[split : split + 2 * NDEV, :] = dots[0][split:] + dots[2][split:]
        part[split + 2 * NDEV :, :] = dots[1][split:] + dots[3][split:]
        for b in range(width // 128):
            cols = slice(b * 128, (b + 1) * 128)
            scores = part[0:split, cols]
            mixed = jnp.where(even, part[split : split + 2 * NDEV, cols], part[split + 2 * NDEV :, cols])
            mixed = mixed.reshape(NZ, 8, 128)
            mixed = (mixed + pltpu.roll(mixed, 7, axis=1)).reshape(2 * NDEV, 128)
            last = jnp.where(even, mixed, NEG)
            peak = jnp.maximum(jnp.max(scores, axis=0, keepdims=True), jnp.max(last, axis=0, keepdims=True))
            scores = scores - peak
            last = jnp.where(even, last - peak, NEG)
            raised = jnp.exp(scores)
            raised_last = jnp.exp(last)
            norm = jnp.sum(raised, axis=0, keepdims=True) + jnp.sum(raised_last, axis=0, keepdims=True)
            inverse = 1.0 / norm
            prob_acc[0:split, :] += raised * inverse
            prob_acc[split:, :] += raised_last * inverse
            log_norm = jnp.log(norm)
            at = pl.ds(pl.multiple_of(me * share + c * width + b * 128, 128), 128)
            codes = []
            for k in range(TOP):
                pick = picks[k : k + 1, at]
                found = jnp.max(jnp.where(pick == ids, scores, NEG), axis=0, keepdims=True)
                found_last = jnp.max(jnp.where(pick == tail_ids, last, NEG), axis=0, keepdims=True)
                codes.append(encode(log_norm, jnp.maximum(found, found_last)))
            for w in range(WORDS):
                gate_msg[me, c, w, b : b + 1, :] = codes[w] + jnp.left_shift(codes[w + WORDS], 16)
            best = scores.reshape(2 * NZ, 8, 128)
            best = jnp.maximum(best, pltpu.roll(best, 7, axis=1))
            best = jnp.maximum(best, pltpu.roll(best, 6, axis=1)).reshape(NZ, 2, 8, 128)
            best = jnp.where(rem(row8, 4) < 2, best[:, 0], pltpu.roll(best[:, 1], 2, axis=1))
            best = jnp.maximum(best, last.reshape(NZ, 8, 128))
            code = encode(log_norm.reshape(1, 1, 128), best)
            if c == 0:
                top_code[:, :, cols] = code
            else:
                words = top_code[:, :, cols] + jnp.left_shift(code, 16)
                for zi in range(NZ):
                    for yi in range(NY):
                        r = 2 * ((yi % 2) * 2 + yi // 2)
                        top_msg[zi * NY + yi, :, cols] = words[zi, r : r + 1, :]
        for j in Z_ORDER:
            gate_z(j, c).start()
        for q in Y_ORDER:
            gate_y(q, 0, c).start()

    def top_copy(i):
        return send(top_msg.at[rem(me + i, NDEV)], top_recv.at[me], ts.at[i], tr.at[i], (dp, rem(me + i, NDEV)))

    def start_top(i, carry):
        top_copy(i).start()
        return carry

    lax.fori_loop(1, NDEV, start_top, 0)
    top_recv[me] = top_msg[me]

    arrive([send(cnt_all.at[yy(q)], cnt_all.at[yy(q)], ks.at[2, q], kr.at[2, q], y_peer(q)) for q in Y_ORDER])
    sums = [jnp.float32(0.0)] * 3
    dev_prob, dev_count, sent = [nil] * NY, [nil] * NY, [nil] * NY
    acc = [jnp.zeros((NZ, 128), jnp.float32)] * 3
    for yi in range(NY):
        table = cnt_all[yi].reshape(NZ, 128)
        lanes = lax.broadcasted_iota(jnp.int32, (NZ, 128), 1)
        dev_prob = jnp.zeros((NZ, 128), jnp.float32)
        dev_count = jnp.zeros((NZ, 1), jnp.float32)
        for e in range(PER):
            cnt = jnp.sum(jnp.where(lanes == e, table, nil), axis=1, keepdims=True)
            if e < PER - 1:
                prob = prob_acc[pl.ds(yi * 4 + e, NZ, stride=16), :]
            else:
                prob = prob_acc[pl.ds(4 * NDEV + 2 * ((yi % 2) * 2 + yi // 2), NZ, stride=8), :]
            acc[0] = acc[0] + prob * cnt
            dev_prob = dev_prob + prob
            dev_count = dev_count + cnt
        acc[1] = acc[1] + dev_prob * dev_count
        acc[2] = acc[2] + dev_prob * jnp.sum(jnp.where(lanes == PER, table, nil), axis=1, keepdims=True)
    experts = NDEV * PER
    scale = (experts / (TOP * total) / total, experts / (TOP * total) / PER / total, NDEV / (DEV_TOP * total) / total)
    result = jnp.zeros((1, 128), jnp.float32)
    for i in range(3):
        result = jnp.where(lane == i, whole(acc[i]) * scale[i], result)
    bal_dp[dp] = result
    bal_copies = [send(bal_dp.at[dp], bal_dp.at[dp], bs.at[0, i], br.at[0, i], dp_peer(i)) for i in range(1, NDP)]
    start(bal_copies)

    def show(src, c):
        words = gate_msg[src, c]
        low, high = low_half(words), high_half(words)
        for b in range(width // 128):
            cols = pl.ds(pl.multiple_of(src * share + c * width + b * 128, 128), 128)
            gates[0:WORDS, cols] = low[:, b, :]
            gates[WORDS:TOP, cols] = high[:, b, :]

    for c in range(CHUNKS):
        for j in Z_ORDER:
            gate_z(j, c, False).wait_recv()
            for q in Y_ORDER:
                gate_y(q, j, c).start()
    arrive(bal_copies)
    bal_z[z] = jnp.sum(bal_dp[...], axis=0)
    bal_zs = [send(bal_z.at[z], bal_z.at[z], bs.at[1, j], br.at[1, j], z_peer(j)) for j in range(1, NZ)]
    start(bal_zs)
    for c in range(CHUNKS):
        for j in (0,) + Z_ORDER:
            show(zz(j) * NY + y, c)
    arrive(bal_zs)
    bal_y[y] = jnp.sum(bal_z[...], axis=0)
    bal_ys = [send(bal_y.at[y], bal_y.at[y], bs.at[2, q], br.at[2, q], y_peer(q)) for q in Y_ORDER]
    start(bal_ys)
    for c in range(CHUNKS):
        for j in (0,) + Z_ORDER:
            for q in Y_ORDER:
                gate_y(q, j, c, False).wait_recv()
                show(zz(j) * NY + yy(q), c)

    def show_top(i, carry):
        src = rem(me + NDEV - i, NDEV)

        @pl.when(i > 0)
        def _():
            top_copy(i).wait_recv()

        words = top_recv[src]
        device_max[:, pl.ds(pl.multiple_of(src * share, share), width)] = low_half(words)
        device_max[:, pl.ds(pl.multiple_of(src * share + width, width), width)] = high_half(words)
        return carry

    lax.fori_loop(0, NDEV, show_top, 0)
    arrive(bal_ys)
    balance[...] = jnp.sum(bal_y[...], axis=0)

    for j in Z_ORDER:
        for copy in z_copies(j):
            copy.wait_send()
        for c in range(CHUNKS):
            gate_z(j, c).wait_send()
    for j in (0,) + Z_ORDER:
        for q in Y_ORDER:
            for copy in y_copies(q, j):
                copy.wait_send()
            for c in range(CHUNKS):
                gate_y(q, j, c).wait_send()
        for q in (0,) + Y_ORDER:
            if j or q:
                for copy in core_copies(q, j, core):
                    copy.wait_send()
    for copy in cnt_copies + cnt_z + cnt_y + bal_copies + bal_zs + bal_ys:
        copy.wait_send()

    def sent_top(i, carry):
        top_copy(i).wait_send()
        return carry

    lax.fori_loop(1, NDEV, sent_top, 0)


def put(gate_buf, top_buf, sums, gates, device_max, balance, sem):
    first = pltpu.make_async_copy(gate_buf, gates, sem.at[0])
    second = pltpu.make_async_copy(top_buf, device_max, sem.at[1])
    first.start()
    second.start()
    lane = lax.broadcasted_iota(jnp.int32, (1, 128), 1)
    for i in range(3):
        balance[i] = jnp.sum(jnp.where(lane == i, sums[...], jnp.float32(0.0)))
    first.wait()
    second.wait()


def local(tokens, router, device_pick, expert_pick):
    depth, share = tokens.shape
    width = share // CHUNKS
    dma = pltpu.SemaphoreType.DMA
    f32, i32, bf16 = jnp.float32, jnp.int32, jnp.bfloat16
    outs = (
        jax.ShapeDtypeStruct((TOP, share * NDEV), f32),
        jax.ShapeDtypeStruct((1, share * NDEV), f32),
        jax.ShapeDtypeStruct((1, 128), f32),
    )
    buffers = pl.pallas_call(
        kernel,
        out_shape=outs,
        in_specs=[pl.BlockSpec(memory_space=pltpu.HBM)] * 4,
        out_specs=tuple(pl.BlockSpec(memory_space=pltpu.VMEM) for _ in outs),
        scratch_shapes=[
            pltpu.VMEM((CHUNKS, depth, width), bf16),
            pltpu.VMEM((PER, depth), bf16),
            pltpu.VMEM((TOP, share * NDEV), i32),
            pltpu.VMEM((DEV_TOP, share * NDEV), i32),
            pltpu.VMEM((NDEV, 4, depth), bf16),
            pltpu.VMEM((NDEV, 2, depth // 2), bf16),
            pltpu.VMEM((6 * NDEV, depth), bf16),
            pltpu.VMEM((8 * NDEV, width), f32),
            pltpu.VMEM((6 * NDEV, 128), f32),
            pltpu.VMEM((NZ, 8, width), i32),
            pltpu.VMEM((NDEV, CHUNKS, WORDS, width // 128, 128), i32),
            pltpu.VMEM((NDEV, 1, width), i32),
            pltpu.VMEM((NDEV, 1, width), i32),
            pltpu.VMEM((NDP, 1, 128), f32),
            pltpu.VMEM((NY, NZ, 1, 128), f32),
            pltpu.VMEM((NDP, 1, 128), f32),
            pltpu.VMEM((NZ, 1, 128), f32),
            pltpu.VMEM((NY, 1, 128), f32),
            dma((3,)),
            dma((CHUNKS,)),
            dma((2, NZ)),
            dma((2, NZ)),
            dma((2, NY, NZ)),
            dma((2, NY, NZ)),
            dma((2, NY, NZ)),
            dma((2, NY, NZ)),
            dma((3, NZ)),
            dma((3, NZ)),
            dma((NZ, CHUNKS)),
            dma((NZ, CHUNKS)),
            dma((NY, NZ, CHUNKS)),
            dma((NY, NZ, CHUNKS)),
            dma((NDEV,)),
            dma((NDEV,)),
            dma((3, NZ)),
            dma((3, NZ)),
        ],
        compiler_params=pltpu.CompilerParams(
            collective_id=0, has_side_effects=True, vmem_limit_bytes=62 * 1024 * 1024
        ),
        name="route",
    )(tokens, router.T, device_pick, expert_pick)
    return pl.pallas_call(
        put,
        out_shape=outs[:2] + (jax.ShapeDtypeStruct((3,), f32),),
        in_specs=[pl.BlockSpec(memory_space=pltpu.VMEM)] * 3,
        out_specs=(
            pl.BlockSpec(memory_space=pl.ANY),
            pl.BlockSpec(memory_space=pl.ANY),
            pl.BlockSpec(memory_space=pltpu.SMEM),
        ),
        scratch_shapes=[dma((2,))],
        compiler_params=pltpu.CompilerParams(vmem_limit_bytes=8 * 1024 * 1024),
        name="put",
    )(*buffers)


def solution(mesh):
    placed = (P(None, ("dp", "expert")), P(None, "expert"), P(None, "dp"), P(None, "dp"))
    return jax.shard_map(
        local,
        mesh=mesh,
        in_specs=placed,
        out_specs=(P(None, "dp"), P("expert", "dp"), P()),
        check_vma=False,
    )
```

```python
import jax
import jax.numpy as jnp
from jax import lax
from jax.experimental import pallas as pl
from jax.experimental.pallas import tpu as pltpu
from jax.sharding import PartitionSpec as P

MESH = pl.DeviceIdType.MESH
TOP = 6
DEV_TOP = 3
PER = 5
NX, NZ, NY = 4, 8, 4
NDP = 2 * NX
NDEV = NZ * NY
CODE = 1.4426950408889634 * 2048.0
NEG = -1e30
WORDS = TOP // 2
CHUNKS = 2
VMEM = 67043328
Z_ORDER = (1, 7, 2, 6, 3, 5, 4)
Y_ORDER = (1, 3, 2)


def rem(a, b):
    return lax.rem(a, b)


def encode(log_norm, value):
    return jnp.clip((log_norm - value) * CODE + 0.5, 0.0, 65535.0).astype(jnp.int32)


def low_half(words):
    return jnp.exp2((words & 65535).astype(jnp.float32) * (-1.0 / 2048.0))


def high_half(words):
    return jnp.exp2(lax.shift_right_logical(words, 16).astype(jnp.float32) * (-1.0 / 2048.0))


def kernel(
    tokens, router, expert_pick,
    gates, device_max, balance,
    tok, picks, main, tail, lhs, part, prob_acc, top_code, gate_msg, top_msg, top_recv,
    cnt_dp, cnt_all, bal_plane, bal_dp,
    in_sem, tok_sem, zs, zr, ys, yr, cs, cr, ks, kr, gzs, gzr, gys, gyr, ts, tr, bs, br,
):
    depth, share = tokens.shape
    half, width = depth // 2, share // CHUNKS
    quarter = depth // 4
    total = share * NDEV * NDP
    dp, me = lax.axis_index("dp"), lax.axis_index("expert")
    core, z, y = rem(dp, 2), me // NY, rem(me, NY)
    partner = dp + 1 - 2 * core

    def zz(j):
        return rem(z + NZ - j, NZ)

    def yy(q):
        return rem(y + NY - q, NY)

    def z_peer(j):
        return (dp, rem(z + j, NZ) * NY + y)

    def y_peer(q):
        return (dp, z * NY + rem(y + q, NY))

    def dp_peer(i):
        return (rem(dp + i, NDP), me)

    def send(src, dst, s, r, device):
        return pltpu.make_async_remote_copy(
            src_ref=src, dst_ref=dst, send_sem=s, recv_sem=r, device_id=device, device_id_type=MESH
        )

    pick_copy = pltpu.make_async_copy(expert_pick, picks, in_sem.at[0])
    pick_copy.start()

    def token_copy(c):
        return pltpu.make_async_copy(tokens.at[:, pl.ds(c * width, width)], tok.at[c], tok_sem.at[c])

    for c in range(CHUNKS):
        token_copy(c).start()

    barrier = pltpu.get_barrier_semaphore()
    friends = [z_peer(j) for j in Z_ORDER] + [y_peer(q) for q in Y_ORDER] + [dp_peer(i) for i in range(1, NDP)]
    for device in friends:
        pl.semaphore_signal(barrier, inc=1, device_id=device, device_id_type=MESH)

    def tail_slot(zi, yi):
        return zi * NY + rem(yi, 2) * 2 + yi // 2

    main[me] = router[0:4, :]
    last = router[4:5, :].astype(jnp.float32)
    tail[tail_slot(z, y)] = jnp.concatenate(
        [
            jnp.concatenate([last[:, 0:quarter], last[:, 2 * quarter : 3 * quarter]], axis=1),
            jnp.concatenate([last[:, quarter : 2 * quarter], last[:, 3 * quarter :]], axis=1),
        ],
        axis=0,
    ).astype(jnp.bfloat16)

    pl.semaphore_wait(barrier, len(friends))

    def main_at(zi, yi, c):
        return main.at[zi * NY + yi, :, pl.ds(pl.multiple_of(c * half, half), half)]

    def tail_at(zi, yi, c):
        return tail.at[tail_slot(zi, yi), :, pl.ds(pl.multiple_of(c * quarter, quarter), quarter)]

    def z_copies(j, mine=True):
        zi = z if mine else zz(j)
        return [
            send(f(zi, y, core), f(zi, y, core), zs.at[n, j], zr.at[n, j], z_peer(j))
            for n, f in enumerate((main_at, tail_at))
        ]

    def y_copies(q, j, mine=True):
        yi = y if mine else yy(q)
        return [
            send(f(zz(j), yi, core), f(zz(j), yi, core), ys.at[n, q, j], yr.at[n, q, j], y_peer(q))
            for n, f in enumerate((main_at, tail_at))
        ]

    def core_copies(q, j, c):
        return [
            send(f(zz(j), yy(q), c), f(zz(j), yy(q), c), cs.at[n, q, j], cr.at[n, q, j], (partner, me))
            for n, f in enumerate((main_at, tail_at))
        ]

    def start(copies):
        for copy in copies:
            copy.start()

    def arrive(copies):
        for copy in copies:
            copy.wait_recv()

    for j in Z_ORDER:
        start(z_copies(j))
    for q in Y_ORDER:
        start(y_copies(q, 0))
    pick_copy.wait()
    one, nil = jnp.float32(1.0), jnp.float32(0.0)

    def count(i, counts):
        counts = list(counts)
        for b in range(8):
            cols = pl.ds(pl.multiple_of(i * 1024 + b * 128, 128), 128)
            seen = picks[:, cols] - me * PER
            for e in range(PER):
                counts[e] = counts[e] + jnp.where(seen == e, one, nil)
        return tuple(counts)

    nothing = tuple(jnp.zeros((TOP, 128), jnp.float32) for _ in range(PER))
    counts = lax.fori_loop(0, share * NDEV // 1024, count, nothing)
    lane = lax.broadcasted_iota(jnp.int32, (1, 128), 1)

    def whole(v):
        return jnp.sum(jnp.sum(v, axis=0, keepdims=True), axis=1, keepdims=True)

    mine = jnp.zeros((1, 128), jnp.float32)
    for e in range(PER):
        mine = jnp.where(lane == e, whole(counts[e]), mine)
    cnt_dp[dp] = mine

    cnt_copies = [send(cnt_dp.at[dp], cnt_dp.at[dp], ks.at[0, i], kr.at[0, i], dp_peer(i)) for i in range(1, NDP)]
    start(cnt_copies)
    for j in Z_ORDER:
        arrive(z_copies(j, False))
        for q in Y_ORDER:
            start(y_copies(q, j))
        start(core_copies(0, j, core))

    arrive(cnt_copies)
    cnt_all[y, z] = jnp.sum(cnt_dp[...], axis=0)
    for q in Y_ORDER:
        arrive(y_copies(q, 0, False))
        start(core_copies(q, 0, core))
    cnt_z = [send(cnt_all.at[y, z], cnt_all.at[y, z], ks.at[1, j], kr.at[1, j], z_peer(j)) for j in range(1, NZ)]
    start(cnt_z)
    for n, j in enumerate(Z_ORDER):
        for q in Y_ORDER:
            arrive(y_copies(q, j, False))
            start(core_copies(q, j, core))
        if n == 4:
            arrive([send(cnt_all.at[y, zz(j)], cnt_all.at[y, zz(j)], ks.at[1, j], kr.at[1, j], z_peer(j)) for j in range(1, NZ)])
            cnt_y = [send(cnt_all.at[y], cnt_all.at[y], ks.at[2, q], kr.at[2, q], y_peer(q)) for q in Y_ORDER]
            start(cnt_y)
    split = 4 * NDEV
    block = 512

    def half_of(h):
        return core if h == 0 else 1 - core

    def gather_rows(h):
        lanes = half_of(h) * half
        for i in range(half // block):
            piece = main[:, :, pl.ds(pl.multiple_of(lanes + i * block, 128), block)]
            lhs[h, 0:split, i * block : (i + 1) * block] = piece.reshape(split, block)
        lanes = half_of(h) * quarter
        for i in range(quarter // 256):
            piece = tail[:, :, pl.ds(pl.multiple_of(lanes + i * 256, 128), 256)].reshape(2 * NDEV, 256)
            for s in range(2):
                lhs[h, split:, s * quarter + i * 256 : s * quarter + (i + 1) * 256] = piece

    def dots(h, c):
        return [
            jnp.dot(
                lhs[h, :, s * quarter : (s + 1) * quarter],
                tok[c, pl.ds(pl.multiple_of(half_of(h) * half + s * quarter, 128), quarter), :],
                preferred_element_type=jnp.float32,
            )
            for s in range(2)
        ]

    gather_rows(0)
    for c in range(CHUNKS):
        token_copy(c).wait()
        first, second = dots(0, c)
        part[c, 0:split, :] = first[:split] + second[:split]
        part[c, split : split + 2 * NDEV, :] = first[split:]
        part[c, split + 2 * NDEV :, :] = second[split:]

    for j in (0,) + Z_ORDER:
        for q in (0,) + Y_ORDER:
            if j or q:
                arrive(core_copies(q, j, 1 - core))
    gather_rows(1)

    row = lax.broadcasted_iota(jnp.int32, (4 * NDEV, 128), 0)
    ids = (row // 4) * PER + rem(row, 4)
    trow = lax.broadcasted_iota(jnp.int32, (2 * NDEV, 128), 0)
    tdev = (trow // 8) * NY + rem(trow // 2, 2) * 2 + rem(trow // 4, 2)
    even = rem(trow, 2) == 0
    tail_ids = jnp.where(even, tdev * PER + PER - 1, -1)
    row8 = lax.broadcasted_iota(jnp.int32, (NZ, 8, 128), 1)
    prob_acc[...] = jnp.zeros((6 * NDEV, 128), jnp.float32)

    def gate_at(src, c):
        return gate_msg.at[src, c]

    def gate_z(j, c, mine=True):
        src = me if mine else zz(j) * NY + y
        return send(gate_at(src, c), gate_at(src, c), gzs.at[j, c], gzr.at[j, c], z_peer(j))

    def gate_y(q, j, c, mine=True):
        src = zz(j) * NY + (y if mine else yy(q))
        return send(gate_at(src, c), gate_at(src, c), gys.at[q, j, c], gyr.at[q, j, c], y_peer(q))

    for c in range(CHUNKS):
        first, second = dots(1, c)
        part[c, 0:split, :] += first[:split] + second[:split]
        part[c, split : split + 2 * NDEV, :] += first[split:]
        part[c, split + 2 * NDEV :, :] += second[split:]
        for b in range(width // 128):
            cols = slice(b * 128, (b + 1) * 128)
            scores = part[c, 0:split, cols]
            mixed = jnp.where(even, part[c, split : split + 2 * NDEV, cols], part[c, split + 2 * NDEV :, cols])
            mixed = mixed.reshape(NZ, 8, 128)
            mixed = (mixed + pltpu.roll(mixed, 7, axis=1)).reshape(2 * NDEV, 128)
            last = jnp.where(even, mixed, NEG)
            peak = jnp.maximum(jnp.max(scores, axis=0, keepdims=True), jnp.max(last, axis=0, keepdims=True))
            scores = scores - peak
            last = jnp.where(even, last - peak, NEG)
            raised = jnp.exp(scores)
            raised_last = jnp.exp(last)
            norm = jnp.sum(raised, axis=0, keepdims=True) + jnp.sum(raised_last, axis=0, keepdims=True)
            inverse = 1.0 / norm
            prob_acc[0:split, :] += raised * inverse
            prob_acc[split:, :] += raised_last * inverse
            log_norm = jnp.log(norm)
            at = pl.ds(pl.multiple_of(me * share + c * width + b * 128, 128), 128)
            codes = []
            for k in range(TOP):
                pick = picks[k : k + 1, at]
                found = jnp.max(jnp.where(pick == ids, scores, NEG), axis=0, keepdims=True)
                found_last = jnp.max(jnp.where(pick == tail_ids, last, NEG), axis=0, keepdims=True)
                codes.append(encode(log_norm, jnp.maximum(found, found_last)))
            for w in range(WORDS):
                gate_msg[me, c, w, b : b + 1, :] = codes[w] + jnp.left_shift(codes[w + WORDS], 16)
            best = scores.reshape(2 * NZ, 8, 128)
            best = jnp.maximum(best, pltpu.roll(best, 7, axis=1))
            best = jnp.maximum(best, pltpu.roll(best, 6, axis=1)).reshape(NZ, 2, 8, 128)
            best = jnp.where(rem(row8, 4) < 2, best[:, 0], pltpu.roll(best[:, 1], 2, axis=1))
            best = jnp.maximum(best, last.reshape(NZ, 8, 128))
            code = encode(log_norm.reshape(1, 1, 128), best)
            if c == 0:
                top_code[:, :, cols] = code
            else:
                words = top_code[:, :, cols] + jnp.left_shift(code, 16)
                for zi in range(NZ):
                    for yi in range(NY):
                        r = 2 * ((yi % 2) * 2 + yi // 2)
                        top_msg[zi * NY + yi, :, cols] = words[zi, r : r + 1, :]
        for j in Z_ORDER:
            gate_z(j, c).start()
        for q in Y_ORDER:
            gate_y(q, 0, c).start()

    arrive([send(cnt_all.at[yy(q)], cnt_all.at[yy(q)], ks.at[2, q], kr.at[2, q], y_peer(q)) for q in Y_ORDER])
    acc = [jnp.zeros((NZ, 128), jnp.float32)] * 3
    for yi in range(NY):
        table = cnt_all[yi].reshape(NZ, 128)
        lanes = lax.broadcasted_iota(jnp.int32, (NZ, 128), 1)
        dev_prob = jnp.zeros((NZ, 128), jnp.float32)
        dev_count = jnp.zeros((NZ, 1), jnp.float32)
        for e in range(PER):
            cnt = jnp.sum(jnp.where(lanes == e, table, nil), axis=1, keepdims=True)
            if e < PER - 1:
                prob = prob_acc[pl.ds(yi * 4 + e, NZ, stride=16), :]
            else:
                prob = prob_acc[pl.ds(4 * NDEV + 2 * ((yi % 2) * 2 + yi // 2), NZ, stride=8), :]
            acc[0] = acc[0] + prob * cnt
            dev_prob = dev_prob + prob
            dev_count = dev_count + cnt
        acc[1] = acc[1] + dev_prob * dev_count
        acc[2] = acc[2] + dev_prob * (dev_count * 0.5)
    experts = NDEV * PER
    scale = (experts / (TOP * total) / total, experts / (TOP * total) / PER / total, NDEV / (DEV_TOP * total) / total)
    result = jnp.zeros((1, 128), jnp.float32)
    for i in range(3):
        result = jnp.where(lane == i, whole(acc[i]) * scale[i], result)
    bal_plane[me] = result

    def plane_copy(i):
        return send(bal_plane.at[me], bal_plane.at[me], bs.at[0, i], br.at[0, i], (dp, rem(me + i, NDEV)))

    def start_plane(i, carry):
        plane_copy(i).start()
        return carry

    lax.fori_loop(1, NDEV, start_plane, 0)

    def top_copy(i):
        return send(top_msg.at[rem(me + i, NDEV)], top_recv.at[me], ts.at[i], tr.at[i], (dp, rem(me + i, NDEV)))

    def start_top(i, carry):
        top_copy(i).start()
        return carry

    lax.fori_loop(1, NDEV, start_top, 0)
    top_recv[me] = top_msg[me]

    def show(src, c):
        words = gate_msg[src, c]
        low, high = low_half(words), high_half(words)
        for b in range(width // 128):
            cols = pl.ds(pl.multiple_of(src * share + c * width + b * 128, 128), 128)
            gates[0:WORDS, cols] = low[:, b, :]
            gates[WORDS:TOP, cols] = high[:, b, :]

    for c in range(CHUNKS):
        for j in Z_ORDER:
            gate_z(j, c, False).wait_recv()
            for q in Y_ORDER:
                gate_y(q, j, c).start()
    for c in range(CHUNKS):
        for j in (0,) + Z_ORDER:
            show(zz(j) * NY + y, c)

    def take_plane(i, carry):
        plane_copy(i).wait_recv()
        return carry

    lax.fori_loop(1, NDEV, take_plane, 0)
    bal_dp[dp] = jnp.sum(bal_plane[...], axis=0)
    bal_copies = [send(bal_dp.at[dp], bal_dp.at[dp], bs.at[1, i], br.at[1, i], dp_peer(i)) for i in range(1, NDP)]
    start(bal_copies)
    for j in (0,) + Z_ORDER:
        for copy in z_copies(j) if j else ():
            copy.wait_send()
        for q in (0,) + Y_ORDER:
            for copy in (y_copies(q, j) if q else []) + (core_copies(q, j, core) if j or q else []):
                copy.wait_send()
    for copy in cnt_copies + cnt_z + cnt_y:
        copy.wait_send()
    for c in range(CHUNKS):
        for j in (0,) + Z_ORDER:
            for q in Y_ORDER:
                gate_y(q, j, c, False).wait_recv()
                show(zz(j) * NY + yy(q), c)

    def show_top(i, carry):
        src = rem(me + NDEV - i, NDEV)

        @pl.when(i > 0)
        def _():
            top_copy(i).wait_recv()

        words = top_recv[src]
        device_max[:, pl.ds(pl.multiple_of(src * share, share), width)] = low_half(words)
        device_max[:, pl.ds(pl.multiple_of(src * share + width, width), width)] = high_half(words)
        return carry

    lax.fori_loop(0, NDEV, show_top, 0)
    arrive(bal_copies)
    balance[...] = jnp.sum(bal_dp[...], axis=0)

    for j in (0,) + Z_ORDER:
        for c in range(CHUNKS):
            if j:
                gate_z(j, c).wait_send()
            for q in Y_ORDER:
                gate_y(q, j, c).wait_send()
    for copy in bal_copies:
        copy.wait_send()

    def sent_top(i, carry):
        top_copy(i).wait_send()
        plane_copy(i).wait_send()
        return carry

    lax.fori_loop(1, NDEV, sent_top, 0)


def put(gate_buf, top_buf, sums, gates, device_max, balance, sem):
    first = pltpu.make_async_copy(gate_buf, gates, sem.at[0])
    second = pltpu.make_async_copy(top_buf, device_max, sem.at[1])
    first.start()
    second.start()
    lane = lax.broadcasted_iota(jnp.int32, (1, 128), 1)
    for i in range(3):
        balance[i] = jnp.sum(jnp.where(lane == i, sums[...], jnp.float32(0.0)))
    first.wait()
    second.wait()


def local(tokens, router, device_pick, expert_pick):
    depth, share = tokens.shape
    width = share // CHUNKS
    dma = pltpu.SemaphoreType.DMA
    f32, i32, bf16 = jnp.float32, jnp.int32, jnp.bfloat16
    outs = (
        jax.ShapeDtypeStruct((TOP, share * NDEV), f32),
        jax.ShapeDtypeStruct((1, share * NDEV), f32),
        jax.ShapeDtypeStruct((1, 128), f32),
    )
    buffers = pl.pallas_call(
        kernel,
        out_shape=outs,
        in_specs=[pl.BlockSpec(memory_space=s) for s in (pltpu.HBM, pltpu.VMEM, pltpu.HBM)],
        out_specs=tuple(pl.BlockSpec(memory_space=pltpu.VMEM) for _ in outs),
        scratch_shapes=[
            pltpu.VMEM((CHUNKS, depth, width), bf16),
            pltpu.VMEM((TOP, share * NDEV), i32),
            pltpu.VMEM((NDEV, 4, depth), bf16),
            pltpu.VMEM((NDEV, 2, depth // 2), bf16),
            pltpu.VMEM((2, 6 * NDEV, depth // 2), bf16),
            pltpu.VMEM((CHUNKS, 8 * NDEV, width), f32),
            pltpu.VMEM((6 * NDEV, 128), f32),
            pltpu.VMEM((NZ, 8, width), i32),
            pltpu.VMEM((NDEV, CHUNKS, WORDS, width // 128, 128), i32),
            pltpu.VMEM((NDEV, 1, width), i32),
            pltpu.VMEM((NDEV, 1, width), i32),
            pltpu.VMEM((NDP, 1, 128), f32),
            pltpu.VMEM((NY, NZ, 1, 128), f32),
            pltpu.VMEM((NDEV, 1, 128), f32),
            pltpu.VMEM((NDP, 1, 128), f32),
            dma((1,)),
            dma((CHUNKS,)),
            dma((2, NZ)),
            dma((2, NZ)),
            dma((2, NY, NZ)),
            dma((2, NY, NZ)),
            dma((2, NY, NZ)),
            dma((2, NY, NZ)),
            dma((3, NZ)),
            dma((3, NZ)),
            dma((NZ, CHUNKS)),
            dma((NZ, CHUNKS)),
            dma((NY, NZ, CHUNKS)),
            dma((NY, NZ, CHUNKS)),
            dma((NDEV,)),
            dma((NDEV,)),
            dma((2, NDEV)),
            dma((2, NDEV)),
        ],
        compiler_params=pltpu.CompilerParams(
            collective_id=0, has_side_effects=True, vmem_limit_bytes=VMEM - 12058624
        ),
        name="route",
    )(tokens, router.T, expert_pick)
    return pl.pallas_call(
        put,
        out_shape=outs[:2] + (jax.ShapeDtypeStruct((3,), f32),),
        in_specs=[pl.BlockSpec(memory_space=pltpu.VMEM)] * 3,
        out_specs=(
            pl.BlockSpec(memory_space=pl.ANY),
            pl.BlockSpec(memory_space=pl.ANY),
            pl.BlockSpec(memory_space=pltpu.SMEM),
        ),
        scratch_shapes=[dma((2,))],
        compiler_params=pltpu.CompilerParams(vmem_limit_bytes=8 * 1024 * 1024),
        name="put",
    )(*buffers)


def solution(mesh):
    placed = (P(None, ("dp", "expert")), P(None, "expert"), P(None, "dp"), P(None, "dp"))
    return jax.shard_map(
        local,
        mesh=mesh,
        in_specs=placed,
        out_specs=(P(None, "dp"), P("expert", "dp"), P()),
        check_vma=False,
    )
```

```python
import jax
import jax.numpy as jnp
from jax import lax
from jax.experimental import pallas as pl
from jax.experimental.pallas import tpu as pltpu
from jax.sharding import PartitionSpec as P

MESH = pl.DeviceIdType.MESH
TOP = 6
DEV_TOP = 3
PER = 5
NX, NZ, NY = 4, 8, 4
NDP = 2 * NX
NDEV = NZ * NY
CODE = 1.4426950408889634 * 2048.0
NEG = -1e30
WORDS = TOP // 2
CHUNKS = 2
VMEM = 67043328
Z_ORDER = (1, 7, 2, 6, 3, 5, 4)
Y_ORDER = (1, 3, 2)


def rem(a, b):
    return lax.rem(a, b)


def encode(log_norm, value):
    return jnp.clip((log_norm - value) * CODE + 0.5, 0.0, 65535.0).astype(jnp.int32)


def low_half(words):
    return jnp.exp2((words & 65535).astype(jnp.float32) * (-1.0 / 2048.0))


def high_half(words):
    return jnp.exp2(lax.shift_right_logical(words, 16).astype(jnp.float32) * (-1.0 / 2048.0))


def kernel(
    tokens, router, expert_pick,
    gates, device_max, balance,
    tok, picks, main, tail, lhs, part, prob_acc, top_code, gate_msg, top_msg, top_recv,
    cnt_dp, cnt_all, bal_plane, bal_dp,
    in_sem, tok_sem, zs, zr, ys, yr, cs, cr, ks, kr, gzs, gzr, gys, gyr, ts, tr, bs, br,
):
    depth, share = tokens.shape
    half, width = depth // 2, share // CHUNKS
    quarter = depth // 4
    total = share * NDEV * NDP
    dp, me = lax.axis_index("dp"), lax.axis_index("expert")
    core, z, y = rem(dp, 2), me // NY, rem(me, NY)
    partner = dp + 1 - 2 * core

    def zz(j):
        return rem(z + NZ - j, NZ)

    def yy(q):
        return rem(y + NY - q, NY)

    def z_peer(j):
        return (dp, rem(z + j, NZ) * NY + y)

    def y_peer(q):
        return (dp, z * NY + rem(y + q, NY))

    def dp_peer(i):
        return (rem(dp + i, NDP), me)

    def send(src, dst, s, r, device):
        return pltpu.make_async_remote_copy(
            src_ref=src, dst_ref=dst, send_sem=s, recv_sem=r, device_id=device, device_id_type=MESH
        )

    pick_copy = pltpu.make_async_copy(expert_pick, picks, in_sem.at[0])
    pick_copy.start()

    def token_copy(c):
        return pltpu.make_async_copy(tokens.at[:, pl.ds(c * width, width)], tok.at[c], tok_sem.at[c])

    for c in range(CHUNKS):
        token_copy(c).start()

    barrier = pltpu.get_barrier_semaphore()
    friends = [z_peer(j) for j in Z_ORDER] + [y_peer(q) for q in Y_ORDER] + [dp_peer(i) for i in range(1, NDP)]
    for device in friends:
        pl.semaphore_signal(barrier, inc=1, device_id=device, device_id_type=MESH)

    def tail_slot(zi, yi):
        return zi * NY + rem(yi, 2) * 2 + yi // 2

    main[me] = router[0:4, :]
    last = router[4:5, :].astype(jnp.float32)
    tail[tail_slot(z, y)] = jnp.concatenate(
        [
            jnp.concatenate([last[:, 0:quarter], last[:, 2 * quarter : 3 * quarter]], axis=1),
            jnp.concatenate([last[:, quarter : 2 * quarter], last[:, 3 * quarter :]], axis=1),
        ],
        axis=0,
    ).astype(jnp.bfloat16)

    pl.semaphore_wait(barrier, len(friends))

    def main_at(zi, yi, c):
        return main.at[zi * NY + yi, :, pl.ds(pl.multiple_of(c * half, half), half)]

    def tail_at(zi, yi, c):
        return tail.at[tail_slot(zi, yi), :, pl.ds(pl.multiple_of(c * quarter, quarter), quarter)]

    def z_copies(j, mine=True):
        zi = z if mine else zz(j)
        return [
            send(f(zi, y, core), f(zi, y, core), zs.at[n, j], zr.at[n, j], z_peer(j))
            for n, f in enumerate((main_at, tail_at))
        ]

    def y_copies(q, j, mine=True):
        yi = y if mine else yy(q)
        return [
            send(f(zz(j), yi, core), f(zz(j), yi, core), ys.at[n, q, j], yr.at[n, q, j], y_peer(q))
            for n, f in enumerate((main_at, tail_at))
        ]

    def core_copies(q, j, c):
        return [
            send(f(zz(j), yy(q), c), f(zz(j), yy(q), c), cs.at[n, q, j], cr.at[n, q, j], (partner, me))
            for n, f in enumerate((main_at, tail_at))
        ]

    def start(copies):
        for copy in copies:
            copy.start()

    def arrive(copies):
        for copy in copies:
            copy.wait_recv()

    for j in Z_ORDER:
        start(z_copies(j))
    for q in Y_ORDER:
        start(y_copies(q, 0))
    pick_copy.wait()
    one, nil = jnp.float32(1.0), jnp.float32(0.0)

    def count(i, counts):
        counts = list(counts)
        for b in range(8):
            cols = pl.ds(pl.multiple_of(i * 1024 + b * 128, 128), 128)
            seen = picks[:, cols] - me * PER
            for e in range(PER):
                counts[e] = counts[e] + jnp.where(seen == e, one, nil)
        return tuple(counts)

    nothing = tuple(jnp.zeros((TOP, 128), jnp.float32) for _ in range(PER))
    counts = lax.fori_loop(0, share * NDEV // 1024, count, nothing)
    lane = lax.broadcasted_iota(jnp.int32, (1, 128), 1)

    def whole(v):
        return jnp.sum(jnp.sum(v, axis=0, keepdims=True), axis=1, keepdims=True)

    mine = jnp.zeros((1, 128), jnp.float32)
    for e in range(PER):
        mine = jnp.where(lane == e, whole(counts[e]), mine)
    cnt_dp[dp] = mine

    cnt_copies = [send(cnt_dp.at[dp], cnt_dp.at[dp], ks.at[0, i], kr.at[0, i], dp_peer(i)) for i in range(1, NDP)]
    start(cnt_copies)
    for j in Z_ORDER:
        arrive(z_copies(j, False))
        for q in Y_ORDER:
            start(y_copies(q, j))
        start(core_copies(0, j, core))

    arrive(cnt_copies)
    cnt_all[y, z] = jnp.sum(cnt_dp[...], axis=0)
    for q in Y_ORDER:
        arrive(y_copies(q, 0, False))
        start(core_copies(q, 0, core))
    cnt_z = [send(cnt_all.at[y, z], cnt_all.at[y, z], ks.at[1, j], kr.at[1, j], z_peer(j)) for j in range(1, NZ)]
    start(cnt_z)
    for n, j in enumerate(Z_ORDER):
        for q in Y_ORDER:
            arrive(y_copies(q, j, False))
            start(core_copies(q, j, core))
        if n == 4:
            arrive([send(cnt_all.at[y, zz(j)], cnt_all.at[y, zz(j)], ks.at[1, j], kr.at[1, j], z_peer(j)) for j in range(1, NZ)])
            cnt_y = [send(cnt_all.at[y], cnt_all.at[y], ks.at[2, q], kr.at[2, q], y_peer(q)) for q in Y_ORDER]
            start(cnt_y)
    split = 4 * NDEV
    block = 512

    def half_of(h):
        return core if h == 0 else 1 - core

    def gather_rows(h):
        lanes = half_of(h) * half
        for i in range(half // block):
            piece = main[:, :, pl.ds(pl.multiple_of(lanes + i * block, 128), block)]
            lhs[h, 0:split, i * block : (i + 1) * block] = piece.reshape(split, block)
        lanes = half_of(h) * quarter
        for i in range(quarter // 256):
            piece = tail[:, :, pl.ds(pl.multiple_of(lanes + i * 256, 128), 256)].reshape(2 * NDEV, 256)
            for s in range(2):
                lhs[h, split:, s * quarter + i * 256 : s * quarter + (i + 1) * 256] = piece

    def dots(h, c):
        return [
            jnp.dot(
                lhs[h, :, s * quarter : (s + 1) * quarter],
                tok[c, pl.ds(pl.multiple_of(half_of(h) * half + s * quarter, 128), quarter), :],
                preferred_element_type=jnp.float32,
            )
            for s in range(2)
        ]

    gather_rows(0)
    for c in range(CHUNKS):
        token_copy(c).wait()
        first, second = dots(0, c)
        part[c, 0:split, :] = first[:split] + second[:split]
        part[c, split : split + 2 * NDEV, :] = first[split:]
        part[c, split + 2 * NDEV :, :] = second[split:]

    for j in (0,) + Z_ORDER:
        for q in (0,) + Y_ORDER:
            if j or q:
                arrive(core_copies(q, j, 1 - core))
    gather_rows(1)

    row = lax.broadcasted_iota(jnp.int32, (4 * NDEV, 128), 0)
    ids = (row // 4) * PER + rem(row, 4)
    trow = lax.broadcasted_iota(jnp.int32, (2 * NDEV, 128), 0)
    tdev = (trow // 8) * NY + rem(trow // 2, 2) * 2 + rem(trow // 4, 2)
    even = rem(trow, 2) == 0
    tail_ids = jnp.where(even, tdev * PER + PER - 1, -1)
    row8 = lax.broadcasted_iota(jnp.int32, (NZ, 8, 128), 1)
    prob_acc[...] = jnp.zeros((6 * NDEV, 128), jnp.float32)

    def gate_at(src, c):
        return gate_msg.at[src, c]

    def gate_z(j, c, mine=True):
        src = me if mine else zz(j) * NY + y
        return send(gate_at(src, c), gate_at(src, c), gzs.at[j, c], gzr.at[j, c], z_peer(j))

    def gate_y(q, j, c, mine=True):
        src = zz(j) * NY + (y if mine else yy(q))
        return send(gate_at(src, c), gate_at(src, c), gys.at[q, j, c], gyr.at[q, j, c], y_peer(q))

    for c in range(CHUNKS):
        first, second = dots(1, c)
        part[c, 0:split, :] += first[:split] + second[:split]
        part[c, split : split + 2 * NDEV, :] += first[split:]
        part[c, split + 2 * NDEV :, :] += second[split:]
        for b in range(width // 128):
            cols = slice(b * 128, (b + 1) * 128)
            scores = part[c, 0:split, cols]
            mixed = jnp.where(even, part[c, split : split + 2 * NDEV, cols], part[c, split + 2 * NDEV :, cols])
            mixed = mixed.reshape(NZ, 8, 128)
            mixed = (mixed + pltpu.roll(mixed, 7, axis=1)).reshape(2 * NDEV, 128)
            last = jnp.where(even, mixed, NEG)
            peak = jnp.maximum(jnp.max(scores, axis=0, keepdims=True), jnp.max(last, axis=0, keepdims=True))
            scores = scores - peak
            last = jnp.where(even, last - peak, NEG)
            raised = jnp.exp(scores)
            raised_last = jnp.exp(last)
            norm = jnp.sum(raised, axis=0, keepdims=True) + jnp.sum(raised_last, axis=0, keepdims=True)
            inverse = 1.0 / norm
            prob_acc[0:split, :] += raised * inverse
            prob_acc[split:, :] += raised_last * inverse
            log_norm = jnp.log(norm)
            at = pl.ds(pl.multiple_of(me * share + c * width + b * 128, 128), 128)
            codes = []
            for k in range(TOP):
                pick = picks[k : k + 1, at]
                found = jnp.max(jnp.where(pick == ids, scores, NEG), axis=0, keepdims=True)
                found_last = jnp.max(jnp.where(pick == tail_ids, last, NEG), axis=0, keepdims=True)
                codes.append(encode(log_norm, jnp.maximum(found, found_last)))
            for w in range(WORDS):
                gate_msg[me, c, w, b : b + 1, :] = codes[w] + jnp.left_shift(codes[w + WORDS], 16)
            best = scores.reshape(2 * NZ, 8, 128)
            best = jnp.maximum(best, pltpu.roll(best, 7, axis=1))
            best = jnp.maximum(best, pltpu.roll(best, 6, axis=1)).reshape(NZ, 2, 8, 128)
            best = jnp.where(rem(row8, 4) < 2, best[:, 0], pltpu.roll(best[:, 1], 2, axis=1))
            best = jnp.maximum(best, last.reshape(NZ, 8, 128))
            code = encode(log_norm.reshape(1, 1, 128), best)
            if c == 0:
                top_code[:, :, cols] = code
            else:
                words = top_code[:, :, cols] + jnp.left_shift(code, 16)
                for zi in range(NZ):
                    for yi in range(NY):
                        r = 2 * ((yi % 2) * 2 + yi // 2)
                        top_msg[zi * NY + yi, :, cols] = words[zi, r : r + 1, :]
        for j in Z_ORDER:
            gate_z(j, c).start()
        for q in Y_ORDER:
            gate_y(q, 0, c).start()

    arrive([send(cnt_all.at[yy(q)], cnt_all.at[yy(q)], ks.at[2, q], kr.at[2, q], y_peer(q)) for q in Y_ORDER])
    acc = [jnp.zeros((NZ, 128), jnp.float32)] * 3
    for yi in range(NY):
        table = cnt_all[yi].reshape(NZ, 128)
        lanes = lax.broadcasted_iota(jnp.int32, (NZ, 128), 1)
        dev_prob = jnp.zeros((NZ, 128), jnp.float32)
        dev_count = jnp.zeros((NZ, 1), jnp.float32)
        for e in range(PER):
            cnt = jnp.sum(jnp.where(lanes == e, table, nil), axis=1, keepdims=True)
            if e < PER - 1:
                prob = prob_acc[pl.ds(yi * 4 + e, NZ, stride=16), :]
            else:
                prob = prob_acc[pl.ds(4 * NDEV + 2 * ((yi % 2) * 2 + yi // 2), NZ, stride=8), :]
            acc[0] = acc[0] + prob * cnt
            dev_prob = dev_prob + prob
            dev_count = dev_count + cnt
        acc[1] = acc[1] + dev_prob * dev_count
        acc[2] = acc[2] + dev_prob * (dev_count * 0.5)
    experts = NDEV * PER
    scale = (experts / (TOP * total) / total, experts / (TOP * total) / PER / total, NDEV / (DEV_TOP * total) / total)
    result = jnp.zeros((1, 128), jnp.float32)
    for i in range(3):
        result = jnp.where(lane == i, whole(acc[i]) * scale[i], result)
    bal_plane[dp * NY + y] = result

    def plane_copy(i):
        at = bal_plane.at[dp * NY + y]
        return send(at, at, bs.at[0, i], br.at[0, i], (rem(dp + rem(i, NDP), NDP), z * NY + rem(y + i // NDP, NY)))

    def start_plane(i, carry):
        plane_copy(i).start()
        return carry

    lax.fori_loop(1, NDEV, start_plane, 0)

    def top_copy(i):
        return send(top_msg.at[rem(me + i, NDEV)], top_recv.at[me], ts.at[i], tr.at[i], (dp, rem(me + i, NDEV)))

    def start_top(i, carry):
        top_copy(i).start()
        return carry

    lax.fori_loop(1, NDEV, start_top, 0)
    top_recv[me] = top_msg[me]

    def show(src, c):
        words = gate_msg[src, c]
        low, high = low_half(words), high_half(words)
        for b in range(width // 128):
            cols = pl.ds(pl.multiple_of(src * share + c * width + b * 128, 128), 128)
            gates[0:WORDS, cols] = low[:, b, :]
            gates[WORDS:TOP, cols] = high[:, b, :]

    for c in range(CHUNKS):
        for j in Z_ORDER:
            gate_z(j, c, False).wait_recv()
            for q in Y_ORDER:
                gate_y(q, j, c).start()
    def take_plane(i, carry):
        plane_copy(i).wait_recv()
        return carry

    lax.fori_loop(1, NDEV, take_plane, 0)
    bal_dp[z] = jnp.sum(bal_plane[...], axis=0)
    bal_copies = [send(bal_dp.at[z], bal_dp.at[z], bs.at[1, j], br.at[1, j], z_peer(j)) for j in range(1, NZ)]
    start(bal_copies)
    for c in range(CHUNKS):
        for j in (0,) + Z_ORDER:
            show(zz(j) * NY + y, c)

    for j in (0,) + Z_ORDER:
        for copy in z_copies(j) if j else ():
            copy.wait_send()
        for q in (0,) + Y_ORDER:
            for copy in (y_copies(q, j) if q else []) + (core_copies(q, j, core) if j or q else []):
                copy.wait_send()
    for copy in cnt_copies + cnt_z + cnt_y:
        copy.wait_send()
    def take_gates(c):
        for j in (0,) + Z_ORDER:
            for q in Y_ORDER:
                gate_y(q, j, c, False).wait_recv()
                show(zz(j) * NY + yy(q), c)

    def gates_sent(c):
        for j in (0,) + Z_ORDER:
            if j:
                gate_z(j, c).wait_send()
            for q in Y_ORDER:
                gate_y(q, j, c).wait_send()

    for c in range(CHUNKS - 1):
        take_gates(c)
        gates_sent(c)

    def show_top(i, carry):
        src = rem(me + NDEV - i, NDEV)

        @pl.when(i > 0)
        def _():
            top_copy(i).wait_recv()

        words = top_recv[src]
        device_max[:, pl.ds(pl.multiple_of(src * share, share), width)] = low_half(words)
        device_max[:, pl.ds(pl.multiple_of(src * share + width, width), width)] = high_half(words)
        return carry

    lax.fori_loop(0, NDEV, show_top, 0)
    def sent_top(i, carry):
        top_copy(i).wait_send()
        plane_copy(i).wait_send()
        return carry

    lax.fori_loop(1, NDEV, sent_top, 0)
    take_gates(CHUNKS - 1)
    gates_sent(CHUNKS - 1)
    arrive(bal_copies)
    balance[...] = jnp.sum(bal_dp[...], axis=0)
    for copy in bal_copies:
        copy.wait_send()


def put(gate_buf, top_buf, sums, gates, device_max, balance, sem):
    first = pltpu.make_async_copy(gate_buf, gates, sem.at[0])
    second = pltpu.make_async_copy(top_buf, device_max, sem.at[1])
    first.start()
    second.start()
    lane = lax.broadcasted_iota(jnp.int32, (1, 128), 1)
    for i in range(3):
        balance[i] = jnp.sum(jnp.where(lane == i, sums[...], jnp.float32(0.0)))
    first.wait()
    second.wait()


def local(tokens, router, device_pick, expert_pick):
    depth, share = tokens.shape
    width = share // CHUNKS
    dma = pltpu.SemaphoreType.DMA
    f32, i32, bf16 = jnp.float32, jnp.int32, jnp.bfloat16
    outs = (
        jax.ShapeDtypeStruct((TOP, share * NDEV), f32),
        jax.ShapeDtypeStruct((1, share * NDEV), f32),
        jax.ShapeDtypeStruct((1, 128), f32),
    )
    buffers = pl.pallas_call(
        kernel,
        out_shape=outs,
        in_specs=[pl.BlockSpec(memory_space=s) for s in (pltpu.HBM, pltpu.VMEM, pltpu.HBM)],
        out_specs=tuple(pl.BlockSpec(memory_space=pltpu.VMEM) for _ in outs),
        scratch_shapes=[
            pltpu.VMEM((CHUNKS, depth, width), bf16),
            pltpu.VMEM((TOP, share * NDEV), i32),
            pltpu.VMEM((NDEV, 4, depth), bf16),
            pltpu.VMEM((NDEV, 2, depth // 2), bf16),
            pltpu.VMEM((2, 6 * NDEV, depth // 2), bf16),
            pltpu.VMEM((CHUNKS, 8 * NDEV, width), f32),
            pltpu.VMEM((6 * NDEV, 128), f32),
            pltpu.VMEM((NZ, 8, width), i32),
            pltpu.VMEM((NDEV, CHUNKS, WORDS, width // 128, 128), i32),
            pltpu.VMEM((NDEV, 1, width), i32),
            pltpu.VMEM((NDEV, 1, width), i32),
            pltpu.VMEM((NDP, 1, 128), f32),
            pltpu.VMEM((NY, NZ, 1, 128), f32),
            pltpu.VMEM((NDEV, 1, 128), f32),
            pltpu.VMEM((NDP, 1, 128), f32),
            dma((1,)),
            dma((CHUNKS,)),
            dma((2, NZ)),
            dma((2, NZ)),
            dma((2, NY, NZ)),
            dma((2, NY, NZ)),
            dma((2, NY, NZ)),
            dma((2, NY, NZ)),
            dma((3, NZ)),
            dma((3, NZ)),
            dma((NZ, CHUNKS)),
            dma((NZ, CHUNKS)),
            dma((NY, NZ, CHUNKS)),
            dma((NY, NZ, CHUNKS)),
            dma((NDEV,)),
            dma((NDEV,)),
            dma((2, NDEV)),
            dma((2, NDEV)),
        ],
        compiler_params=pltpu.CompilerParams(
            collective_id=0, has_side_effects=True, vmem_limit_bytes=VMEM - 12058624
        ),
        name="route",
    )(tokens, router.T, expert_pick)
    return pl.pallas_call(
        put,
        out_shape=outs[:2] + (jax.ShapeDtypeStruct((3,), f32),),
        in_specs=[pl.BlockSpec(memory_space=pltpu.VMEM)] * 3,
        out_specs=(
            pl.BlockSpec(memory_space=pl.ANY),
            pl.BlockSpec(memory_space=pl.ANY),
            pl.BlockSpec(memory_space=pltpu.SMEM),
        ),
        scratch_shapes=[dma((2,))],
        compiler_params=pltpu.CompilerParams(vmem_limit_bytes=8 * 1024 * 1024),
        name="put",
    )(*buffers)


def solution(mesh):
    placed = (P(None, ("dp", "expert")), P(None, "expert"), P(None, "dp"), P(None, "dp"))
    return jax.shard_map(
        local,
        mesh=mesh,
        in_specs=placed,
        out_specs=(P(None, "dp"), P("expert", "dp"), P()),
        check_vma=False,
    )
```

```python
import jax
import jax.numpy as jnp
from jax import lax
from jax.experimental import pallas as pl
from jax.experimental.pallas import tpu as pltpu
from jax.sharding import PartitionSpec as P

MESH = pl.DeviceIdType.MESH
TOP = 6
DEV_TOP = 3
PER = 5
NX, NZ, NY = 4, 8, 4
NDP = 2 * NX
NDEV = NZ * NY
CODE = 1.4426950408889634 * 2048.0
NEG = -1e30
WORDS = TOP // 2
CHUNKS = 2
VMEM = 67043328
Z_ORDER = (1, 7, 2, 6, 3, 5, 4)
Y_ORDER = (1, 3, 2)


def rem(a, b):
    return lax.rem(a, b)


def encode(log_norm, value):
    return jnp.clip((log_norm - value) * CODE + 0.5, 0.0, 65535.0).astype(jnp.int32)


def low_half(words):
    return jnp.exp2((words & 65535).astype(jnp.float32) * (-1.0 / 2048.0))


def high_half(words):
    return jnp.exp2(lax.shift_right_logical(words, 16).astype(jnp.float32) * (-1.0 / 2048.0))


def kernel(
    tokens, router, expert_pick,
    gates, device_max, balance,
    tok, picks, main, tail, lhs, part, prob_acc, top_code, gate_msg, top_msg, top_recv,
    cnt_dp, cnt_all, bal_plane, bal_dp,
    in_sem, tok_sem, zs, zr, ys, yr, cs, cr, ks, kr, gzs, gzr, gys, gyr, ts, tr, bs, br,
):
    depth, share = tokens.shape
    half, width = depth // 2, share // CHUNKS
    quarter = depth // 4
    total = share * NDEV * NDP
    dp, me = lax.axis_index("dp"), lax.axis_index("expert")
    core, z, y = rem(dp, 2), me // NY, rem(me, NY)
    partner = dp + 1 - 2 * core

    def zz(j):
        return rem(z + NZ - j, NZ)

    def yy(q):
        return rem(y + NY - q, NY)

    def z_peer(j):
        return (dp, rem(z + j, NZ) * NY + y)

    def y_peer(q):
        return (dp, z * NY + rem(y + q, NY))

    def dp_peer(i):
        return (rem(dp + i, NDP), me)

    def send(src, dst, s, r, device):
        return pltpu.make_async_remote_copy(
            src_ref=src, dst_ref=dst, send_sem=s, recv_sem=r, device_id=device, device_id_type=MESH
        )

    barrier = pltpu.get_barrier_semaphore()
    friends = [z_peer(j) for j in (4, 3, 5, 2, 6, 1, 7)] + [y_peer(q) for q in Y_ORDER] + [dp_peer(i) for i in range(1, NDP)]
    for device in friends:
        pl.semaphore_signal(barrier, inc=1, device_id=device, device_id_type=MESH)

    pick_copy = pltpu.make_async_copy(expert_pick, picks, in_sem.at[0])
    pick_copy.start()

    def token_copy(c):
        return pltpu.make_async_copy(tokens.at[:, pl.ds(c * width, width)], tok.at[c], tok_sem.at[c])

    for c in range(CHUNKS):
        token_copy(c).start()

    def tail_slot(zi, yi):
        return zi * NY + rem(yi, 2) * 2 + yi // 2

    main[me] = router[0:4, :]
    last = router[4:5, :].astype(jnp.float32)
    tail[tail_slot(z, y)] = jnp.concatenate(
        [
            jnp.concatenate([last[:, 0:quarter], last[:, 2 * quarter : 3 * quarter]], axis=1),
            jnp.concatenate([last[:, quarter : 2 * quarter], last[:, 3 * quarter :]], axis=1),
        ],
        axis=0,
    ).astype(jnp.bfloat16)

    pl.semaphore_wait(barrier, len(friends))

    def main_at(zi, yi, c):
        return main.at[zi * NY + yi, :, pl.ds(pl.multiple_of(c * half, half), half)]

    def tail_at(zi, yi, c):
        return tail.at[tail_slot(zi, yi), :, pl.ds(pl.multiple_of(c * quarter, quarter), quarter)]

    def z_copies(j, mine=True):
        zi = z if mine else zz(j)
        return [
            send(f(zi, y, core), f(zi, y, core), zs.at[n, j], zr.at[n, j], z_peer(j))
            for n, f in enumerate((main_at, tail_at))
        ]

    def y_copies(q, j, mine=True):
        yi = y if mine else yy(q)
        return [
            send(f(zz(j), yi, core), f(zz(j), yi, core), ys.at[n, q, j], yr.at[n, q, j], y_peer(q))
            for n, f in enumerate((main_at, tail_at))
        ]

    def core_copies(q, j, c):
        return [
            send(f(zz(j), yy(q), c), f(zz(j), yy(q), c), cs.at[n, q, j], cr.at[n, q, j], (partner, me))
            for n, f in enumerate((main_at, tail_at))
        ]

    def start(copies):
        for copy in copies:
            copy.start()

    def arrive(copies):
        for copy in copies:
            copy.wait_recv()

    for j in Z_ORDER:
        start(z_copies(j))
    for q in Y_ORDER:
        start(y_copies(q, 0))
    pick_copy.wait()
    one, nil = jnp.float32(1.0), jnp.float32(0.0)

    def count(i, counts):
        counts = list(counts)
        for b in range(8):
            cols = pl.ds(pl.multiple_of(i * 1024 + b * 128, 128), 128)
            seen = picks[:, cols] - me * PER
            for e in range(PER):
                counts[e] = counts[e] + jnp.where(seen == e, one, nil)
        return tuple(counts)

    nothing = tuple(jnp.zeros((TOP, 128), jnp.float32) for _ in range(PER))
    counts = lax.fori_loop(0, share * NDEV // 1024, count, nothing)
    lane = lax.broadcasted_iota(jnp.int32, (1, 128), 1)

    def whole(v):
        return jnp.sum(jnp.sum(v, axis=0, keepdims=True), axis=1, keepdims=True)

    mine = jnp.zeros((1, 128), jnp.float32)
    for e in range(PER):
        mine = jnp.where(lane == e, whole(counts[e]), mine)
    cnt_dp[dp] = mine

    cnt_copies = [send(cnt_dp.at[dp], cnt_dp.at[dp], ks.at[0, i], kr.at[0, i], dp_peer(i)) for i in range(1, NDP)]
    start(cnt_copies)
    for j in Z_ORDER:
        arrive(z_copies(j, False))
        for q in Y_ORDER:
            start(y_copies(q, j))
        start(core_copies(0, j, core))

    arrive(cnt_copies)
    cnt_all[y, z] = jnp.sum(cnt_dp[...], axis=0)
    for q in Y_ORDER:
        arrive(y_copies(q, 0, False))
        start(core_copies(q, 0, core))
    cnt_z = [send(cnt_all.at[y, z], cnt_all.at[y, z], ks.at[1, j], kr.at[1, j], z_peer(j)) for j in range(1, NZ)]
    start(cnt_z)
    for n, j in enumerate(Z_ORDER):
        for q in Y_ORDER:
            arrive(y_copies(q, j, False))
            start(core_copies(q, j, core))
        if n == 4:
            arrive([send(cnt_all.at[y, zz(j)], cnt_all.at[y, zz(j)], ks.at[1, j], kr.at[1, j], z_peer(j)) for j in range(1, NZ)])
            cnt_y = [send(cnt_all.at[y], cnt_all.at[y], ks.at[2, q], kr.at[2, q], y_peer(q)) for q in Y_ORDER]
            start(cnt_y)
    split = 4 * NDEV
    block = 512

    def half_of(h):
        return core if h == 0 else 1 - core

    def gather_rows(h):
        lanes = half_of(h) * half
        for i in range(half // block):
            piece = main[:, :, pl.ds(pl.multiple_of(lanes + i * block, 128), block)]
            lhs[h, 0:split, i * block : (i + 1) * block] = piece.reshape(split, block)
        lanes = half_of(h) * quarter
        for i in range(quarter // 256):
            piece = tail[:, :, pl.ds(pl.multiple_of(lanes + i * 256, 128), 256)].reshape(2 * NDEV, 256)
            for s in range(2):
                lhs[h, split:, s * quarter + i * 256 : s * quarter + (i + 1) * 256] = piece

    def dots(h, c):
        return [
            jnp.dot(
                lhs[h, :, s * quarter : (s + 1) * quarter],
                tok[c, pl.ds(pl.multiple_of(half_of(h) * half + s * quarter, 128), quarter), :],
                preferred_element_type=jnp.float32,
            )
            for s in range(2)
        ]

    gather_rows(0)
    for c in range(CHUNKS):
        token_copy(c).wait()
        first, second = dots(0, c)
        part[c, 0:split, :] = first[:split] + second[:split]
        part[c, split : split + 2 * NDEV, :] = first[split:]
        part[c, split + 2 * NDEV :, :] = second[split:]

    for j in (0,) + Z_ORDER:
        for q in (0,) + Y_ORDER:
            if j or q:
                arrive(core_copies(q, j, 1 - core))
    gather_rows(1)

    row = lax.broadcasted_iota(jnp.int32, (4 * NDEV, 128), 0)
    ids = (row // 4) * PER + rem(row, 4)
    trow = lax.broadcasted_iota(jnp.int32, (2 * NDEV, 128), 0)
    tdev = (trow // 8) * NY + rem(trow // 2, 2) * 2 + rem(trow // 4, 2)
    even = rem(trow, 2) == 0
    tail_ids = jnp.where(even, tdev * PER + PER - 1, -1)
    row8 = lax.broadcasted_iota(jnp.int32, (NZ, 8, 128), 1)
    prob_acc[...] = jnp.zeros((6 * NDEV, 128), jnp.float32)

    def gate_at(src, c):
        return gate_msg.at[src, c]

    def gate_z(j, c, mine=True):
        src = me if mine else zz(j) * NY + y
        return send(gate_at(src, c), gate_at(src, c), gzs.at[j, c], gzr.at[j, c], z_peer(j))

    def gate_y(q, j, c, mine=True):
        src = zz(j) * NY + (y if mine else yy(q))
        return send(gate_at(src, c), gate_at(src, c), gys.at[q, j, c], gyr.at[q, j, c], y_peer(q))

    for c in range(CHUNKS):
        first, second = dots(1, c)
        part[c, 0:split, :] += first[:split] + second[:split]
        part[c, split : split + 2 * NDEV, :] += first[split:]
        part[c, split + 2 * NDEV :, :] += second[split:]
        for b in range(width // 128):
            cols = slice(b * 128, (b + 1) * 128)
            scores = part[c, 0:split, cols]
            mixed = jnp.where(even, part[c, split : split + 2 * NDEV, cols], part[c, split + 2 * NDEV :, cols])
            mixed = mixed.reshape(NZ, 8, 128)
            mixed = (mixed + pltpu.roll(mixed, 7, axis=1)).reshape(2 * NDEV, 128)
            last = jnp.where(even, mixed, NEG)
            peak = jnp.maximum(jnp.max(scores, axis=0, keepdims=True), jnp.max(last, axis=0, keepdims=True))
            scores = scores - peak
            last = jnp.where(even, last - peak, NEG)
            raised = jnp.exp(scores)
            raised_last = jnp.exp(last)
            norm = jnp.sum(raised, axis=0, keepdims=True) + jnp.sum(raised_last, axis=0, keepdims=True)
            inverse = 1.0 / norm
            prob_acc[0:split, :] += raised * inverse
            prob_acc[split:, :] += raised_last * inverse
            log_norm = jnp.log(norm)
            at = pl.ds(pl.multiple_of(me * share + c * width + b * 128, 128), 128)
            codes = []
            for k in range(TOP):
                pick = picks[k : k + 1, at]
                found = jnp.max(jnp.where(pick == ids, scores, NEG), axis=0, keepdims=True)
                found_last = jnp.max(jnp.where(pick == tail_ids, last, NEG), axis=0, keepdims=True)
                codes.append(encode(log_norm, jnp.maximum(found, found_last)))
            for w in range(WORDS):
                gate_msg[me, c, w, b : b + 1, :] = codes[w] + jnp.left_shift(codes[w + WORDS], 16)
            best = scores.reshape(2 * NZ, 8, 128)
            best = jnp.maximum(best, pltpu.roll(best, 7, axis=1))
            best = jnp.maximum(best, pltpu.roll(best, 6, axis=1)).reshape(NZ, 2, 8, 128)
            best = jnp.where(rem(row8, 4) < 2, best[:, 0], pltpu.roll(best[:, 1], 2, axis=1))
            best = jnp.maximum(best, last.reshape(NZ, 8, 128))
            code = encode(log_norm.reshape(1, 1, 128), best)
            if c == 0:
                top_code[:, :, cols] = code
            else:
                words = top_code[:, :, cols] + jnp.left_shift(code, 16)
                for zi in range(NZ):
                    for yi in range(NY):
                        r = 2 * ((yi % 2) * 2 + yi // 2)
                        top_msg[zi * NY + yi, :, cols] = words[zi, r : r + 1, :]
        for j in Z_ORDER:
            gate_z(j, c).start()
        for q in Y_ORDER:
            gate_y(q, 0, c).start()

    arrive([send(cnt_all.at[yy(q)], cnt_all.at[yy(q)], ks.at[2, q], kr.at[2, q], y_peer(q)) for q in Y_ORDER])
    acc = [jnp.zeros((NZ, 128), jnp.float32)] * 3
    for yi in range(NY):
        table = cnt_all[yi].reshape(NZ, 128)
        lanes = lax.broadcasted_iota(jnp.int32, (NZ, 128), 1)
        dev_prob = jnp.zeros((NZ, 128), jnp.float32)
        dev_count = jnp.zeros((NZ, 1), jnp.float32)
        for e in range(PER):
            cnt = jnp.sum(jnp.where(lanes == e, table, nil), axis=1, keepdims=True)
            if e < PER - 1:
                prob = prob_acc[pl.ds(yi * 4 + e, NZ, stride=16), :]
            else:
                prob = prob_acc[pl.ds(4 * NDEV + 2 * ((yi % 2) * 2 + yi // 2), NZ, stride=8), :]
            acc[0] = acc[0] + prob * cnt
            dev_prob = dev_prob + prob
            dev_count = dev_count + cnt
        acc[1] = acc[1] + dev_prob * dev_count
        acc[2] = acc[2] + dev_prob * (dev_count * 0.5)
    experts = NDEV * PER
    scale = (experts / (TOP * total) / total, experts / (TOP * total) / PER / total, NDEV / (DEV_TOP * total) / total)
    result = jnp.zeros((1, 128), jnp.float32)
    for i in range(3):
        result = jnp.where(lane == i, whole(acc[i]) * scale[i], result)
    bal_plane[dp * NY + y] = result

    def plane_copy(i):
        at = bal_plane.at[dp * NY + y]
        return send(at, at, bs.at[0, i], br.at[0, i], (rem(dp + rem(i, NDP), NDP), z * NY + rem(y + i // NDP, NY)))

    def start_plane(i, carry):
        plane_copy(i).start()
        return carry

    lax.fori_loop(1, NDEV, start_plane, 0)

    def top_copy(i):
        return send(top_msg.at[rem(me + i, NDEV)], top_recv.at[me], ts.at[i], tr.at[i], (dp, rem(me + i, NDEV)))

    def start_top(i, carry):
        top_copy(i).start()
        return carry

    lax.fori_loop(1, NDEV, start_top, 0)
    top_recv[me] = top_msg[me]

    def show(src, c):
        words = gate_msg[src, c]
        low, high = low_half(words), high_half(words)
        for b in range(width // 128):
            cols = pl.ds(pl.multiple_of(src * share + c * width + b * 128, 128), 128)
            gates[0:WORDS, cols] = low[:, b, :]
            gates[WORDS:TOP, cols] = high[:, b, :]

    for c in range(CHUNKS):
        for j in Z_ORDER:
            gate_z(j, c, False).wait_recv()
            for q in Y_ORDER:
                gate_y(q, j, c).start()
    def take_plane(i, carry):
        plane_copy(i).wait_recv()
        return carry

    lax.fori_loop(1, NDEV, take_plane, 0)
    bal_dp[z] = jnp.sum(bal_plane[...], axis=0)
    bal_copies = [send(bal_dp.at[z], bal_dp.at[z], bs.at[1, j], br.at[1, j], z_peer(j)) for j in range(1, NZ)]
    start(bal_copies)
    for c in range(CHUNKS):
        for j in (0,) + Z_ORDER:
            show(zz(j) * NY + y, c)

    for j in (0,) + Z_ORDER:
        for copy in z_copies(j) if j else ():
            copy.wait_send()
        for q in (0,) + Y_ORDER:
            for copy in (y_copies(q, j) if q else []) + (core_copies(q, j, core) if j or q else []):
                copy.wait_send()
    for copy in cnt_copies + cnt_z + cnt_y:
        copy.wait_send()
    def take_gates(c):
        for j in (0,) + Z_ORDER:
            for q in Y_ORDER:
                gate_y(q, j, c, False).wait_recv()
                show(zz(j) * NY + yy(q), c)

    def gates_sent(c):
        for j in (0,) + Z_ORDER:
            if j:
                gate_z(j, c).wait_send()
            for q in Y_ORDER:
                gate_y(q, j, c).wait_send()

    for c in range(CHUNKS - 1):
        take_gates(c)
        gates_sent(c)

    def show_top(i, carry):
        src = rem(me + NDEV - i, NDEV)

        @pl.when(i > 0)
        def _():
            top_copy(i).wait_recv()

        words = top_recv[src]
        device_max[:, pl.ds(pl.multiple_of(src * share, share), width)] = low_half(words)
        device_max[:, pl.ds(pl.multiple_of(src * share + width, width), width)] = high_half(words)
        return carry

    lax.fori_loop(0, NDEV, show_top, 0)
    def sent_top(i, carry):
        top_copy(i).wait_send()
        plane_copy(i).wait_send()
        return carry

    lax.fori_loop(1, NDEV, sent_top, 0)
    take_gates(CHUNKS - 1)
    gates_sent(CHUNKS - 1)
    arrive(bal_copies)
    balance[...] = jnp.sum(bal_dp[...], axis=0)
    for copy in bal_copies:
        copy.wait_send()


def put(gate_buf, top_buf, sums, gates, device_max, balance, sem):
    first = pltpu.make_async_copy(gate_buf, gates, sem.at[0])
    second = pltpu.make_async_copy(top_buf, device_max, sem.at[1])
    first.start()
    second.start()
    lane = lax.broadcasted_iota(jnp.int32, (1, 128), 1)
    for i in range(3):
        balance[i] = jnp.sum(jnp.where(lane == i, sums[...], jnp.float32(0.0)))
    first.wait()
    second.wait()


def local(tokens, router, device_pick, expert_pick):
    depth, share = tokens.shape
    width = share // CHUNKS
    dma = pltpu.SemaphoreType.DMA
    f32, i32, bf16 = jnp.float32, jnp.int32, jnp.bfloat16
    outs = (
        jax.ShapeDtypeStruct((TOP, share * NDEV), f32),
        jax.ShapeDtypeStruct((1, share * NDEV), f32),
        jax.ShapeDtypeStruct((1, 128), f32),
    )
    buffers = pl.pallas_call(
        kernel,
        out_shape=outs,
        in_specs=[pl.BlockSpec(memory_space=s) for s in (pltpu.HBM, pltpu.VMEM, pltpu.HBM)],
        out_specs=tuple(pl.BlockSpec(memory_space=pltpu.VMEM) for _ in outs),
        scratch_shapes=[
            pltpu.VMEM((CHUNKS, depth, width), bf16),
            pltpu.VMEM((TOP, share * NDEV), i32),
            pltpu.VMEM((NDEV, 4, depth), bf16),
            pltpu.VMEM((NDEV, 2, depth // 2), bf16),
            pltpu.VMEM((2, 6 * NDEV, depth // 2), bf16),
            pltpu.VMEM((CHUNKS, 8 * NDEV, width), f32),
            pltpu.VMEM((6 * NDEV, 128), f32),
            pltpu.VMEM((NZ, 8, width), i32),
            pltpu.VMEM((NDEV, CHUNKS, WORDS, width // 128, 128), i32),
            pltpu.VMEM((NDEV, 1, width), i32),
            pltpu.VMEM((NDEV, 1, width), i32),
            pltpu.VMEM((NDP, 1, 128), f32),
            pltpu.VMEM((NY, NZ, 1, 128), f32),
            pltpu.VMEM((NDEV, 1, 128), f32),
            pltpu.VMEM((NDP, 1, 128), f32),
            dma((1,)),
            dma((CHUNKS,)),
            dma((2, NZ)),
            dma((2, NZ)),
            dma((2, NY, NZ)),
            dma((2, NY, NZ)),
            dma((2, NY, NZ)),
            dma((2, NY, NZ)),
            dma((3, NZ)),
            dma((3, NZ)),
            dma((NZ, CHUNKS)),
            dma((NZ, CHUNKS)),
            dma((NY, NZ, CHUNKS)),
            dma((NY, NZ, CHUNKS)),
            dma((NDEV,)),
            dma((NDEV,)),
            dma((2, NDEV)),
            dma((2, NDEV)),
        ],
        compiler_params=pltpu.CompilerParams(
            collective_id=0, has_side_effects=True, vmem_limit_bytes=VMEM - 12058624
        ),
        name="route",
    )(tokens, router.T, expert_pick)
    return pl.pallas_call(
        put,
        out_shape=outs[:2] + (jax.ShapeDtypeStruct((3,), f32),),
        in_specs=[pl.BlockSpec(memory_space=pltpu.VMEM)] * 3,
        out_specs=(
            pl.BlockSpec(memory_space=pl.ANY),
            pl.BlockSpec(memory_space=pl.ANY),
            pl.BlockSpec(memory_space=pltpu.SMEM),
        ),
        scratch_shapes=[dma((2,))],
        compiler_params=pltpu.CompilerParams(vmem_limit_bytes=8 * 1024 * 1024),
        name="put",
    )(*buffers)


def solution(mesh):
    placed = (P(None, ("dp", "expert")), P(None, "expert"), P(None, "dp"), P(None, "dp"))
    return jax.shard_map(
        local,
        mesh=mesh,
        in_specs=placed,
        out_specs=(P(None, "dp"), P("expert", "dp"), P()),
        check_vma=False,
    )
```
